32 devices in a mesh: patch: 8 (over z, x), rep: 4 (over y, core).
Axes of the slice: x: 2, y: 2, z: 4, core: 2. Of those that a mesh axis runs over, the one named last changes fastest.
Arguments:
- node_latents: bfloat16 [4, 3072, 512], P('rep', 'patch'), may hold values from -6 to 6
- edge_latents: bfloat16 [4, 10240, 512], P('rep', 'patch'), may hold values from -6 to 6
- targets: bfloat16 [4, 3072, 128], P('rep', 'patch'), may hold values from -6 to 6
- edge_weight_in: bfloat16 [1536, 512], replicated, may hold values from -0.15625 to 0.15625
- edge_weight_out: bfloat16 [512, 512], replicated, may hold values from -0.25 to 0.25
- node_weight_in: bfloat16 [1024, 512], replicated, may hold values from -0.1875 to 0.1875
- node_weight_out: bfloat16 [512, 512], replicated, may hold values from -0.25 to 0.25
- readout_weight: bfloat16 [512, 128], replicated, may hold values from -0.25 to 0.25
- send_rows: int32 [8, 96], P('patch'), may hold values from 0 to 383, as said below
- far_rows: int32 [8, 8], P('patch'), may hold values from 0 to 383, as said below
- edge_sender: int32 [10240], P('patch'), may hold values from 0 to 487
- edge_receiver: int32 [10240], P('patch'), may hold values from 0 to 383
- edge_count: int32 [8], P('patch'), may hold values from 80 to 1280, as said below
- land_mask: int32 [3072], P('patch'), may hold values 0 or 1
- lat_band: int32 [3072], P('patch'), may hold values from 0 to 720
Outputs:
- node_grad: bfloat16 [4, 3072, 512], P('rep', 'patch')
- edge_grad: bfloat16 [4, 10240, 512], P('rep', 'patch')
- grad_edge_in: float32 [1536, 512], P('patch')
- grad_edge_out: float32 [512, 512], P('patch')
- grad_node_in: float32 [1024, 512], P('patch')
- grad_node_out: float32 [512, 512], P('patch')
- grad_readout: float32 [512, 128], P('patch')
The draws below stay inside these ranges and needn't reach their ends.
Inputs may be any that keep to these rules, and one draw needn't show every extreme that they name: `send_rows`: the 16 entries of a patch for one neighbour are distinct. `far_rows`: each patch sends exactly one node to every patch (itself included). `edge_count`: some patch has all 1280 edges live.
All inputs are finite; a program needn't handle non-finite values. No bound on the sum of `land_mask` on one device may be relied on, other than what follows from the above.
Results may differ from the reference program's by a relative error of at most 0.012.
Values may be sent and summed in bfloat16 or wider, within the bound.
A program may use at most 128 MiB of HBM per device.

```python
import jax
import jax.numpy as jnp
from jax import lax

D = 512
VARS = 128
OCEAN = 32
BANDS = 721
NODE_DEV = 384
EDGE_DEV = 1280
SLOT = 16
FAR = 1
PATCHES = 8
REPS = 4
NODES = 3072
EDGES = 10240


def draw_send_rows(key, part):
    patches = EDGES // EDGE_DEV
    scores = jax.random.randint(key, (patches, 6, NODE_DEV), 0, 1 << 16) * NODE_DEV + jnp.arange(NODE_DEV, dtype=jnp.int32)
    order = jnp.argsort(scores, axis=-1, stable=True)[:, :, :SLOT]
    return order.reshape(patches, 6 * SLOT).astype(jnp.int32)


def draw_far_rows(key, part):
    patches = EDGES // EDGE_DEV
    scores = jax.random.randint(key, (patches, patches, NODE_DEV), 0, 1 << 16) * NODE_DEV + jnp.arange(NODE_DEV, dtype=jnp.int32)
    order = jnp.argsort(scores, axis=-1, stable=True)[:, :, :FAR]
    return order.reshape(patches, patches * FAR).astype(jnp.int32)


def draw_edge_sender(key, part):
    patches = EDGES // EDGE_DEV
    kind = jax.random.randint(jax.random.fold_in(key, 1), (EDGES,), 0, 100)
    local = jax.random.randint(jax.random.fold_in(key, 2), (EDGES,), 0, NODE_DEV)
    near = NODE_DEV + jax.random.randint(jax.random.fold_in(key, 3), (EDGES,), 0, 6 * SLOT)
    far = NODE_DEV + 6 * SLOT + jax.random.randint(jax.random.fold_in(key, 4), (EDGES,), 0, FAR * patches)
    return jnp.where(kind < 72, local, jnp.where(kind < 88, near, far)).astype(jnp.int32)


def draw_edge_count(key, part):
    patches = EDGES // EDGE_DEV
    counts = jax.random.randint(key, (patches,), EDGE_DEV // 16, EDGE_DEV + 1)
    fullest = jax.random.randint(jax.random.fold_in(key, 7), (), 0, patches)
    return jnp.where(jnp.arange(patches) == fullest, EDGE_DEV, counts).astype(jnp.int32)


def with_ends(entries, own_key, least, high):
    dims = entries.shape
    spot = [jax.random.randint(jax.random.fold_in(own_key, axis), (), 0, dims[axis]) for axis in range(len(dims))]
    entries = entries.at[tuple(spot)].set(least)
    longest = dims.index(max(dims))
    spot[longest] = (spot[longest] + 1) % dims[longest]
    return entries.at[tuple(spot)].set(high)


def block_levels(rng, extent, pieces, low, high):
    def one(position, parts):
        draws = jax.random.uniform(jax.random.fold_in(jax.random.fold_in(rng, 6), position), (parts,), jnp.float32, low / len(pieces), high / len(pieces))
        return jnp.repeat(jnp.exp(draws), extent[position] // parts).reshape((-1,) + (1,) * (len(extent) - position - 1))

    factor_of = one(*pieces[0])
    for cut in pieces[1:]:
        factor_of = factor_of * one(*cut)
    return factor_of


def normal_values(stream_key, dims, scale, most, split=(), kind=jnp.bfloat16):
    entries = scale * jax.random.normal(stream_key, dims, jnp.float32)
    if split:
        entries = entries * block_levels(stream_key, dims, split, -0.22, 0.18)
    return jnp.clip(entries, -most, most).astype(kind)


def setup_inputs(seed: int = 0) -> dict:
    key_of = jax.random.split(jax.random.key(seed), 16)
    node_latents = normal_values(key_of[0], (REPS, NODES, D), 1.0, 6.0, ((0, 4), (1, 8)))
    edge_latents = normal_values(key_of[1], (REPS, EDGES, D), 1.0, 6.0, ((0, 4), (1, 8)))
    targets = normal_values(key_of[2], (REPS, NODES, VARS), 1.0, 6.0, ((0, 4), (1, 8)))
    edge_weight_in = normal_values(key_of[3], (3 * D, D), (3 * D) ** -0.5, 0.15625)
    edge_weight_out = normal_values(key_of[4], (D, D), D ** -0.5, 0.25)
    node_weight_in = normal_values(key_of[5], (2 * D, D), (2 * D) ** -0.5, 0.1875)
    node_weight_out = normal_values(key_of[6], (D, D), D ** -0.5, 0.25)
    readout_weight = normal_values(key_of[7], (D, VARS), D ** -0.5, 0.25)
    send_rows = draw_send_rows(jax.random.fold_in(key_of[15], 71), 0)
    far_rows = draw_far_rows(jax.random.fold_in(key_of[15], 71), 0)
    edge_sender = draw_edge_sender(jax.random.fold_in(key_of[15], 71), 0)
    edge_receiver = with_ends(jax.random.randint(key_of[11], (EDGES,), 0, NODE_DEV), jax.random.fold_in(key_of[11], 1), 0, NODE_DEV - 1).astype(jnp.int32)
    edge_count = draw_edge_count(jax.random.fold_in(key_of[15], 71), 0)
    land_mask = with_ends((jax.random.randint(key_of[13], (NODES,), 0, 10) < 3).astype(jnp.int32), jax.random.fold_in(key_of[13], 1), 0, 1)
    lat_band = with_ends(jax.random.randint(key_of[14], (NODES,), 0, BANDS), jax.random.fold_in(key_of[14], 1), 0, BANDS - 1).astype(jnp.int32)
    return {"node_latents": node_latents, "edge_latents": edge_latents, "targets": targets, "edge_weight_in": edge_weight_in, "edge_weight_out": edge_weight_out, "node_weight_in": node_weight_in, "node_weight_out": node_weight_out, "readout_weight": readout_weight, "send_rows": send_rows, "far_rows": far_rows, "edge_sender": edge_sender, "edge_receiver": edge_receiver, "edge_count": edge_count, "land_mask": land_mask, "lat_band": lat_band}


def normalize(values):
    average = lax.optimization_barrier(jnp.mean(values, axis=-1, keepdims=True))
    centred = values - average
    variance = lax.optimization_barrier(jnp.mean(centred * centred, axis=-1, keepdims=True))
    inverse = lax.rsqrt(variance + 1e-05)
    return (centred * inverse, inverse)

def norm_back(gradient, normed, inverse):
    first = lax.optimization_barrier(jnp.mean(gradient, axis=-1, keepdims=True))
    second = lax.optimization_barrier(jnp.mean(gradient * normed, axis=-1, keepdims=True))
    return inverse * (gradient - first - normed * second)

def silu_grad(values):
    logistic = jax.nn.sigmoid(values)
    return logistic * (1.0 + values * (1.0 - logistic))

def product(left, right):
    return jnp.dot(left, right, preferred_element_type=jnp.float32)

def product_left(left, right):
    return jnp.dot(left.T, right, preferred_element_type=jnp.float32)

def product_right(left, right):
    return jnp.dot(left, right.T, preferred_element_type=jnp.float32)

def reference(node_latents, edge_latents, targets, edge_weight_in, edge_weight_out, node_weight_in, node_weight_out, readout_weight, send_rows, far_rows, edge_sender, edge_receiver, edge_count, land_mask, lat_band):
    positions = jnp.arange(EDGES, dtype=jnp.int32)
    device = (positions // EDGE_DEV).astype(jnp.int32)
    near_total = 6 * SLOT
    offset = jnp.maximum(edge_sender - NODE_DEV, 0).astype(jnp.int32)
    near_index = jnp.minimum(offset, near_total - 1).astype(jnp.int32)
    neighbour = (near_index // SLOT).astype(jnp.int32)
    distance = ((neighbour // 2 + 1) * (1 - 2 * (neighbour % 2))).astype(jnp.int32)
    near_patch = ((device - distance + PATCHES) % PATCHES).astype(jnp.int32)
    near_node = near_patch * NODE_DEV + send_rows[near_patch, near_index]
    far_index = jnp.maximum(offset - near_total, 0).astype(jnp.int32)
    far_patch = jnp.minimum(far_index // FAR, PATCHES - 1).astype(jnp.int32)
    far_node = far_patch * NODE_DEV + far_rows[far_patch, device * FAR + far_index % FAR]
    remote = jnp.where(offset < near_total, near_node, far_node)
    senders = jnp.where(edge_sender < NODE_DEV, device * NODE_DEV + edge_sender, remote).astype(jnp.int32)
    receivers = (device * NODE_DEV + edge_receiver).astype(jnp.int32)
    alive_mask = (positions % EDGE_DEV < edge_count[device]).astype(jnp.float32)[:, None]
    latitude = -0.5 * jnp.pi + (lat_band.astype(jnp.float32) + 0.5) * (jnp.pi / BANDS)
    area_weight = jnp.cos(latitude)[:, None]
    channel = jnp.arange(VARS, dtype=jnp.int32)
    keep_mask = jnp.where((channel[None, :] < OCEAN) & (land_mask[:, None] == 1), 0.0, 1.0).astype(jnp.float32)
    loss_weight = area_weight * keep_mask
    sums = [jnp.zeros(w.shape, jnp.float32) for w in (edge_weight_in, edge_weight_out, node_weight_in, node_weight_out, readout_weight)]
    node_grads = []
    edge_grads = []
    for replica in range(REPS):
        node_rows = node_latents[replica]
        edge_rows = edge_latents[replica]
        stacked = jnp.concatenate([node_rows[senders], node_rows[receivers], edge_rows], axis=1)
        edge_pre = product(stacked, edge_weight_in)
        edge_hidden = jax.nn.silu(edge_pre).astype(jnp.bfloat16)
        edge_normed, edge_inverse = normalize(product(edge_hidden, edge_weight_out))
        message = (edge_normed * alive_mask).astype(jnp.bfloat16)
        aggregate = jax.ops.segment_sum(message.astype(jnp.float32), receivers, num_segments=NODES).astype(jnp.bfloat16)
        node_input = jnp.concatenate([node_rows, aggregate], axis=1)
        node_pre = product(node_input, node_weight_in)
        node_hidden = jax.nn.silu(node_pre).astype(jnp.bfloat16)
        node_normed, node_inverse = normalize(product(node_hidden, node_weight_out))
        updated = (node_rows.astype(jnp.float32) + node_normed).astype(jnp.bfloat16)
        predicted = product(updated, readout_weight)
        pred_grad = (loss_weight * (predicted - targets[replica].astype(jnp.float32))).astype(jnp.bfloat16)
        updated_grad = product_right(pred_grad, readout_weight)
        node_z_grad = norm_back(updated_grad, node_normed, node_inverse).astype(jnp.bfloat16)
        node_pre_grad = (product_right(node_z_grad, node_weight_out) * silu_grad(node_pre)).astype(jnp.bfloat16)
        input_grad = product_right(node_pre_grad, node_weight_in)
        message_grad = input_grad[:, D:][receivers] * alive_mask
        edge_z_grad = norm_back(message_grad, edge_normed, edge_inverse).astype(jnp.bfloat16)
        edge_pre_grad = (product_right(edge_z_grad, edge_weight_out) * silu_grad(edge_pre)).astype(jnp.bfloat16)
        stacked_grad = product_right(edge_pre_grad, edge_weight_in)
        sender_grad = stacked_grad[:, :D].astype(jnp.bfloat16).astype(jnp.float32)
        receiver_grad = stacked_grad[:, D:2 * D].astype(jnp.bfloat16).astype(jnp.float32)
        edge_grads.append(stacked_grad[:, 2 * D:].astype(jnp.bfloat16))
        total = updated_grad + input_grad[:, :D]
        total = total + jax.ops.segment_sum(sender_grad, senders, num_segments=NODES)
        total = total + jax.ops.segment_sum(receiver_grad, receivers, num_segments=NODES)
        node_grads.append(total.astype(jnp.bfloat16))
        sums[0] = sums[0] + product_left(stacked, edge_pre_grad)
        sums[1] = sums[1] + product_left(edge_hidden, edge_z_grad)
        sums[2] = sums[2] + product_left(node_input, node_pre_grad)
        sums[3] = sums[3] + product_left(node_hidden, node_z_grad)
        sums[4] = sums[4] + product_left(updated, pred_grad)
    factor = 1.0 / (NODES * REPS)
    return (jnp.stack(node_grads), jnp.stack(edge_grads), sums[0] * factor, sums[1] * factor, sums[2] * factor, sums[3] * factor, sums[4] * factor)
```

```python
import functools

import jax
import jax.numpy as jnp
from jax import lax
from jax.experimental import pallas as pl
from jax.experimental.pallas import tpu as pltpu
from jax.sharding import PartitionSpec as P

OCEAN = 32
BANDS = 721
OFFSETS = (1, -1, 2, -2, 3, -3)
MESH = pl.DeviceIdType.MESH
F32 = jnp.float32
BF16 = jnp.bfloat16


def mm(left, right):
    return jnp.dot(left, right, preferred_element_type=F32)


def mm_left(left, right):
    return lax.dot_general(left, right, (((0,), (0,)), ((), ())), preferred_element_type=F32)


def mm_right(left, right):
    return lax.dot_general(left, right, (((1,), (1,)), ((), ())), preferred_element_type=F32)


def logistic(values):
    return 1.0 / (1.0 + jnp.exp(-values))


def mean(values):
    return jnp.mean(values, axis=-1, keepdims=True)


class Stream:
    def __init__(self, refs, sems, split, patch, rep, patches, reps):
        self.own, self.got1, self.acc1, self.got2, self.acc2, self.got3, self.all4, self.fin = refs
        self.send, self.recv = sems
        self.split = split
        self.patch, self.rep, self.patches, self.reps = patch, rep, patches, reps
        self.side = lax.rem(rep, 2)
        self.low, self.high = lax.rem(patch, 2), lax.div(patch, 2)
        self.peer = (patch, rep + 1 - 2 * self.side)
        self.sent = []
        self.wait = []

    def copy(self, src, dst, slot, device):
        c = pltpu.make_async_remote_copy(
            src_ref=src, dst_ref=dst, send_sem=self.send.at[slot], recv_sem=self.recv.at[slot],
            device_id=device, device_id_type=MESH)
        c.start()
        self.sent.append(c)
        self.wait.append(c)

    def arrive(self):
        for c in self.wait:
            c.wait_recv()
        self.wait = []

    def stage1(self):
        src = self.own.at[1 - self.side] if self.split else self.own.at[0]
        self.copy(src, self.got1, 0, self.peer)

    def stage2(self):
        self.arrive()
        mine = self.own[self.side] if self.split else self.own[0]
        self.acc1[...] = (mine.astype(F32) + self.got1[...].astype(F32)).astype(BF16)
        self.copy(self.acc1.at[1 - self.low], self.got2, 1, (self.patch + 1 - 2 * self.low, self.rep))

    def stage3(self):
        self.arrive()
        self.acc2[...] = (self.acc1[self.low].astype(F32) + self.got2[...].astype(F32)).astype(BF16)
        highs = self.patches // 2
        for d in range(1, highs):
            other = lax.rem(self.high + d, highs)
            self.copy(self.acc2.at[other], self.got3.at[d - 1], 1 + d, (2 * other + self.low, self.rep))

    def stage4(self):
        self.arrive()
        highs = self.patches // 2
        total = self.acc2[self.high].astype(F32)
        for d in range(1, highs):
            total = total + self.got3[d - 1].astype(F32)
        rep_highs = self.reps // 2
        here = lax.div(self.rep, 2)
        self.all4[here] = total.astype(BF16)
        for d in range(1, rep_highs):
            other = lax.rem(here + d, rep_highs)
            self.copy(self.all4.at[here], self.all4.at[here], highs + d, (self.patch, 2 * other + self.side))

    def stage5(self, scale):
        self.arrive()
        total = self.all4[0].astype(F32)
        for d in range(1, self.reps // 2):
            total = total + self.all4[d].astype(F32)
        total = total * scale
        if self.split:
            self.fin[self.side] = total
            slot = self.patches // 2 + self.reps // 2
            self.copy(self.fin.at[self.side], self.fin.at[self.side], slot, self.peer)
        else:
            self.fin[0] = total

    def finish(self):
        self.arrive()
        for c in self.sent:
            c.wait_send()


def stream_scratch(rows, width, split, patches, reps):
    highs = patches // 2
    sides = 2 if split else 1
    blocks = (2, highs, rows, width)
    slots = highs + reps // 2 + 1
    return [
        pltpu.VMEM((sides,) + blocks, BF16),
        pltpu.VMEM(blocks, BF16),
        pltpu.VMEM(blocks, BF16),
        pltpu.VMEM(blocks[1:], BF16),
        pltpu.VMEM(blocks[1:], BF16),
        pltpu.VMEM((max(highs - 1, 1), rows, width), BF16),
        pltpu.VMEM((reps // 2, rows, width), BF16),
        pltpu.VMEM((sides, rows, width), F32),
        pltpu.SemaphoreType.DMA((slots,)),
        pltpu.SemaphoreType.DMA((slots,)),
    ]


def put(stream, row, value, patches, split, low=0, rows=None):
    block = value.shape[0] // patches
    rows = block - low if rows is None else rows
    width = value.shape[1] // 2 if split else value.shape[1]
    for p in range(patches):
        for side in range(2 if split else 1):
            stream.own[side, p % 2, p // 2, row : row + rows, :] = value[
                p * block + low : p * block + low + rows, side * width : (side + 1) * width
            ].astype(BF16)


def take(stream, row, rows, out, split):
    if split:
        width = out.shape[1] // 2
        for side in range(2):
            out[:, side * width : (side + 1) * width] = stream.fin[side, row : row + rows, :]
    else:
        out[...] = stream.fin[0, row : row + rows, :]


def kernel(
    dims,
    x, e, tgt, w_ein, w_eout, w_nin, w_nout, w_ro, owners, es, er, count, loss_weight,
    o_node, o_edge, o_ein, o_eout, o_nin, o_nout, o_ro,
    near_out, near_in, far_out, far_in, back_near_out, back_near_in, back_far_out, back_far_in,
    xext, xw, table, sgrad, hid, msg, inv, ezg, epg, agg_grad, total,
    near_send, near_recv, far_send, far_recv, bn_send, bn_recv, bf_send, bf_recv,
    *stream_refs,
):
    patches, reps, slot, far, ext, tile = dims
    nodes, width = x.shape
    edges = e.shape[0]
    near = 6 * slot
    patch, rep = lax.axis_index("patch"), lax.axis_index("rep")
    streams = []
    for i, split in enumerate((True, False, True, True)):
        part = stream_refs[10 * i : 10 * i + 10]
        streams.append(Stream(part[:8], part[8:], split, patch, rep, patches, reps))
    s_node, s_ro, s_one, s_two = streams

    barrier = pltpu.get_barrier_semaphore()
    for d in range(1, patches):
        pl.semaphore_signal(barrier, inc=1, device_id=(lax.rem(patch + d, patches), rep), device_id_type=MESH)
    for d in range(1, reps):
        pl.semaphore_signal(barrier, inc=1, device_id=(patch, lax.rem(rep + d, reps)), device_id_type=MESH)

    own_table = (lax.broadcasted_iota(jnp.int32, (nodes, owners.shape[1]), 0) == owners[...])
    own_table = jnp.where(own_table, 1.0, 0.0).astype(BF16)
    outgoing = mm_left(own_table, x[...])
    for k in range(6):
        near_out[k] = outgoing[k * slot : (k + 1) * slot].astype(BF16)
    for q in range(patches):
        far_out[q] = outgoing[near + q * far : near + (q + 1) * far].astype(BF16)
    pl.semaphore_wait(barrier, patches - 1 + reps - 1)

    def remote(src, dst, send, recv, device):
        c = pltpu.make_async_remote_copy(
            src_ref=src, dst_ref=dst, send_sem=send, recv_sem=recv, device_id=device, device_id_type=MESH)
        c.start()
        return c

    halo = []
    for k, o in enumerate(OFFSETS):
        to = lax.rem(patch + (o + patches), patches)
        halo.append(remote(near_out.at[k], near_in.at[k], near_send.at[k], near_recv.at[k], (to, rep)))
    for d in range(1, patches):
        to = lax.rem(patch + d, patches)
        halo.append(remote(far_out.at[to], far_in.at[patch], far_send.at[d - 1], far_recv.at[d - 1], (to, rep)))
    far_in[patch] = far_out[patch]

    w_s, w_r, w_e = (w_ein.at[pl.ds(i * width, width)] for i in range(3))
    xext[0:nodes, :] = x[...]
    xw[0:nodes, :] = mm(x[...], w_s[...]).astype(BF16)
    xw[ext : ext + nodes, :] = mm(x[...], w_r[...]).astype(BF16)

    def tables(t, _):
        at = pl.ds(pl.multiple_of(t * tile, tile), tile)
        hit = lax.broadcasted_iota(jnp.int32, (ext, tile), 0) == es[:, at]
        table[0:ext, at] = jnp.where(hit, 1.0, 0.0).astype(BF16)
        alive = lax.broadcasted_iota(jnp.int32, (1, tile), 1) + t * tile < count[0]
        ids = jnp.where(alive, er[:, at], -1)
        hit = lax.broadcasted_iota(jnp.int32, (nodes, tile), 0) == ids
        table[ext : ext + nodes, at] = jnp.where(hit, 1.0, 0.0).astype(BF16)
        sgrad[at, :] = mm(e[at, :], w_e[...])
        return 0

    lax.fori_loop(0, edges // tile, tables, 0)

    for c in halo:
        c.wait_recv()
    pieces = [near_in[k] for k in range(6)] + [far_in[q] for q in range(patches)]
    pad = ext - nodes - near - patches * far
    if pad:
        pieces.append(jnp.zeros((pad, width), BF16))
    arrived = jnp.concatenate([v.astype(F32) for v in pieces], axis=0).astype(BF16)
    xext[nodes:ext, :] = arrived
    xw[nodes:ext, :] = mm(arrived, w_s[...]).astype(BF16)

    def edge_forward(t, _):
        at = pl.ds(pl.multiple_of(t * tile, tile), tile)
        pre = sgrad[at, :] + mm_left(table[:, at], xw[...])
        s = logistic(pre)
        hidden = (pre * s).astype(BF16)
        sgrad[at, :] = s * (1.0 + pre * (1.0 - s))
        hid[at, :] = hidden
        z = mm(hidden, w_eout[...])
        centred = z - mean(z)
        inverse = lax.rsqrt(mean(centred * centred) + 1e-05)
        inv[at, :] = inverse
        msg[at, :] = (centred * inverse).astype(BF16)
        return 0

    lax.fori_loop(0, edges // tile, edge_forward, 0)

    aggregate = mm(table[ext : ext + nodes, :], msg[...]).astype(BF16)
    node_pre = mm(x[...], w_nin[0:width, :]) + mm(aggregate, w_nin[width : 2 * width, :])
    s = logistic(node_pre)
    node_hidden = (node_pre * s).astype(BF16)
    node_sgrad = s * (1.0 + node_pre * (1.0 - s))
    z = mm(node_hidden, w_nout[...])
    centred = z - mean(z)
    inverse = lax.rsqrt(mean(centred * centred) + 1e-05)
    normed = centred * inverse
    updated = (x[...].astype(F32) + normed).astype(BF16)
    pred_grad = (loss_weight[...] * (mm(updated, w_ro[...]) - tgt[...].astype(F32))).astype(BF16)
    up_grad = mm_right(pred_grad, w_ro[...])
    z_grad = (inverse * (up_grad - mean(up_grad) - normed * mean(up_grad * normed))).astype(BF16)
    pre_grad = (mm_right(z_grad, w_nout[...]) * node_sgrad).astype(BF16)
    total[...] = up_grad + mm_right(pre_grad, w_nin[0:width, :])
    agg_grad[...] = mm_right(pre_grad, w_nin[width : 2 * width, :]).astype(BF16)
    nin_rows = 2 * width // patches
    put_in = jnp.concatenate([mm_left(x[...], pre_grad), mm_left(aggregate, pre_grad)], axis=0)
    put(s_node, 0, put_in, patches, True)
    put(s_node, nin_rows, mm_left(node_hidden, z_grad), patches, True)
    put(s_ro, 0, mm_left(updated, pred_grad), patches, False)
    s_node.stage1()
    s_ro.stage1()

    def edge_backward(t, _):
        at = pl.ds(pl.multiple_of(t * tile, tile), tile)
        g = mm_left(table[ext : ext + nodes, at], agg_grad[...])
        y = msg[at, :].astype(F32)
        zg = (inv[at, :] * (g - mean(g) - y * mean(g * y))).astype(BF16)
        ezg[at, :] = zg
        epg[at, :] = (mm_right(zg, w_eout[...]) * sgrad[at, :]).astype(BF16)
        return 0

    steps = edges // tile
    first, second = (2 * steps) // 5, (4 * steps) // 5
    lax.fori_loop(0, first, edge_backward, 0)
    s_node.stage2()
    s_ro.stage2()
    lax.fori_loop(first, steps, edge_backward, 0)

    sums32 = mm(table[0:ext, :], epg[...])
    sums = sums32.astype(BF16)
    for k in range(6):
        back_near_out[k] = sums32[nodes + k * slot : nodes + (k + 1) * slot].astype(BF16)
    for q in range(patches):
        at = nodes + near + q * far
        back_far_out[q] = sums32[at : at + far].astype(BF16)
    back = []
    for k, o in enumerate(OFFSETS):
        to = lax.rem(patch + (patches - o), patches)
        back.append(remote(back_near_out.at[k], back_near_in.at[k], bn_send.at[k], bn_recv.at[k], (to, rep)))
    for d in range(1, patches):
        to = lax.rem(patch + d, patches)
        back.append(remote(back_far_out.at[to], back_far_in.at[patch], bf_send.at[d - 1], bf_recv.at[d - 1], (to, rep)))
    back_far_in[patch] = back_far_out[patch]
    share = width // patches
    rsums = mm(table[ext : ext + nodes, :], epg[...]).astype(BF16)
    put_in = jnp.concatenate(
        [mm_left(xext[...], sums), mm_left(x[...], rsums), mm_left(e[...], epg[...])], axis=0)
    put(s_one, 0, put_in, patches, True, 0, share)
    put(s_one, share, mm_left(hid[...], ezg[...]), patches, True)
    s_one.stage1()
    put(s_two, 0, put_in, patches, True, share)
    s_two.stage1()
    s_node.stage3()
    s_ro.stage3()
    s_one.stage2()
    total[...] += mm_right(rsums, w_r[...])

    def edge_out(t, _):
        at = pl.ds(pl.multiple_of(t * tile, tile), tile)
        o_edge[at, :] = mm_right(epg[at, :], w_e[...]).astype(BF16)
        return 0

    s_two.stage2()
    lax.fori_loop(0, first, edge_out, 0)
    s_node.stage4()
    s_ro.stage4()
    lax.fori_loop(first, steps, edge_out, 0)
    for c in back:
        c.wait_recv()
    pieces = [back_near_in[k] for k in range(6)] + [back_far_in[q] for q in range(patches)]
    pad = owners.shape[1] - near - patches * far
    if pad:
        pieces.append(jnp.zeros((pad, width), BF16))
    returned = jnp.concatenate([v.astype(F32) for v in pieces], axis=0).astype(BF16)
    owned = (mm(own_table, returned) + sums32[0:nodes]).astype(BF16)
    o_node[...] = (total[...] + mm_right(owned, w_s[...])).astype(BF16)

    scale = 1.0 / (nodes * patches * reps)
    s_one.stage3()
    s_two.stage3()
    s_node.stage5(scale)
    s_ro.stage5(scale)
    s_one.stage4()
    s_two.stage4()
    s_one.stage5(scale)
    s_two.stage5(scale)
    for c in halo + back:
        c.wait_send()
    s_node.finish()
    s_ro.finish()
    take(s_node, 0, nin_rows, o_nin, True)
    take(s_node, nin_rows, share, o_nout, True)
    take(s_ro, 0, share, o_ro, False)
    s_one.finish()
    take_rows(s_one, 0, share, o_ein, 0)
    take(s_one, share, share, o_eout, True)
    s_two.finish()
    take_rows(s_two, 0, 2 * share, o_ein, share)


def take_rows(stream, row, rows, out, at):
    width = out.shape[1] // 2
    for side in range(2):
        out[at : at + rows, side * width : (side + 1) * width] = stream.fin[side, row : row + rows, :]


def call(
    node_latents, edge_latents, targets, edge_weight_in, edge_weight_out, node_weight_in, node_weight_out,
    readout_weight, send_rows, far_rows, edge_sender, edge_receiver, edge_count, land_mask, lat_band,
):
    nodes, width = node_latents.shape[1:]
    edges = edge_latents.shape[1]
    variables = targets.shape[2]
    patches, reps = lax.axis_size("patch"), lax.axis_size("rep")
    slot = send_rows.shape[1] // 6
    far = far_rows.shape[1] // patches
    near = 6 * slot
    remote_rows = near + patches * far
    ext = -(-(nodes + remote_rows) // 16) * 16
    tile = 256 if edges % 256 == 0 else 128
    listed = -(-remote_rows // 128) * 128
    owners = jnp.concatenate(
        [send_rows[0], far_rows[0], jnp.full((listed - remote_rows,), -1, jnp.int32)])[None]
    latitude = -0.5 * jnp.pi + (lat_band.astype(F32) + 0.5) * (jnp.pi / BANDS)
    channel = lax.iota(jnp.int32, variables)
    keep = jnp.where((channel[None, :] < OCEAN) & (land_mask[:, None] == 1), 0.0, 1.0)
    loss_weight = jnp.cos(latitude)[:, None] * keep
    share = width // patches
    vmem = pl.BlockSpec(memory_space=pltpu.VMEM)
    smem = pl.BlockSpec(memory_space=pltpu.SMEM)
    dma = lambda n: pltpu.SemaphoreType.DMA((n,))
    scratch = [
        pltpu.VMEM((6, slot, width), BF16), pltpu.VMEM((6, slot, width), BF16),
        pltpu.VMEM((patches, far, width), BF16), pltpu.VMEM((patches, far, width), BF16),
        pltpu.VMEM((6, slot, width), BF16), pltpu.VMEM((6, slot, width), BF16),
        pltpu.VMEM((patches, far, width), BF16), pltpu.VMEM((patches, far, width), BF16),
        pltpu.VMEM((ext, width), BF16),
        pltpu.VMEM((ext + nodes, width), BF16),
        pltpu.VMEM((ext + nodes, edges), BF16),
        pltpu.VMEM((edges, width), F32),
        pltpu.VMEM((edges, width), BF16),
        pltpu.VMEM((edges, width), BF16),
        pltpu.VMEM((edges, 1), F32),
        pltpu.VMEM((edges, width), BF16),
        pltpu.VMEM((edges, width), BF16),
        pltpu.VMEM((nodes, width), BF16),
        pltpu.VMEM((nodes, width), F32),
        dma(6), dma(6), dma(patches - 1), dma(patches - 1),
        dma(6), dma(6), dma(patches - 1), dma(patches - 1),
    ]
    scratch += stream_scratch(3 * share, width // 2, True, patches, reps)
    scratch += stream_scratch(share, variables, False, patches, reps)
    scratch += stream_scratch(2 * share, width // 2, True, patches, reps)
    scratch += stream_scratch(2 * share, width // 2, True, patches, reps)
    shape = jax.ShapeDtypeStruct
    outs = pl.pallas_call(
        functools.partial(kernel, (patches, reps, slot, far, ext, tile)),
        out_shape=(
            shape((nodes, width), BF16), shape((edges, width), BF16),
            shape((3 * share, width), F32), shape((share, width), F32),
            shape((2 * share, width), F32), shape((share, width), F32), shape((share, variables), F32),
        ),
        in_specs=[vmem] * 11 + [smem, vmem],
        out_specs=tuple([vmem] * 7),
        scratch_shapes=scratch,
        compiler_params=pltpu.CompilerParams(
            collective_id=0, has_side_effects=True, vmem_limit_bytes=62 * 1024 * 1024),
    )(
        node_latents[0], edge_latents[0], targets[0], edge_weight_in, edge_weight_out, node_weight_in,
        node_weight_out, readout_weight, owners, edge_sender[None], edge_receiver[None], edge_count, loss_weight,
    )
    return (outs[0][None], outs[1][None]) + tuple(outs[2:])


def solution(mesh):
    rows = P("rep", "patch", None)
    in_specs = (rows,) * 3 + (P(),) * 5 + (P("patch", None),) * 2 + (P("patch"),) * 5
    out_specs = (rows,) * 2 + (P("patch", None),) * 5
    return jax.shard_map(call, mesh=mesh, in_specs=in_specs, out_specs=out_specs, check_vma=False)
```

```python
import functools

import jax
import jax.numpy as jnp
from jax import lax
from jax.experimental import pallas as pl
from jax.experimental.pallas import tpu as pltpu
from jax.sharding import PartitionSpec as P

OCEAN = 32
BANDS = 721
OFFSETS = (1, -1, 2, -2, 3, -3)
MESH = pl.DeviceIdType.MESH
F32 = jnp.float32
BF16 = jnp.bfloat16


def mm(left, right):
    return jnp.dot(left, right, preferred_element_type=F32)


def mm_left(left, right):
    return lax.dot_general(left, right, (((0,), (0,)), ((), ())), preferred_element_type=F32)


def mm_right(left, right):
    return lax.dot_general(left, right, (((1,), (1,)), ((), ())), preferred_element_type=F32)


def logistic(values):
    return 1.0 / (1.0 + jnp.exp(-values))


def mean(values):
    return jnp.mean(values, axis=-1, keepdims=True)


class Stream:
    def __init__(self, refs, order, sizes, patch, rep):
        self.order = order
        n = len(order)
        self.own, self.got, self.acc, self.fin = refs[0], refs[1 : 1 + n], refs[1 + n : 1 + 2 * n], refs[1 + 2 * n]
        self.send, self.recv = refs[2 + 2 * n :]
        self.sizes = sizes
        self.patch, self.rep = patch, rep
        self.at = {"side": lax.rem(rep, 2), "wide": lax.div(rep, 2), "low": lax.rem(patch, 2), "high": lax.div(patch, 2)}
        self.reps = sizes["side"] * sizes["wide"]
        self.sent, self.wait, self.slot, self.done = [], [], 0, 0

    def device(self, axis, index):
        at = dict(self.at)
        at[axis] = index
        return (2 * at["high"] + at["low"], 2 * at["wide"] + at["side"])

    def copy(self, src, dst, device):
        c = pltpu.make_async_remote_copy(
            src_ref=src, dst_ref=dst, send_sem=self.send.at[self.slot], recv_sem=self.recv.at[self.slot],
            device_id=device, device_id_type=MESH)
        c.start()
        self.slot += 1
        self.sent.append(c)
        self.wait.append(c)

    def arrive(self):
        for c in self.wait:
            c.wait_recv()
        self.wait = []

    def step(self):
        now, stages = self.done, len(self.order)
        held = self.own
        if now:
            self.arrive()
            axis = self.order[now - 1]
            before = self.own if now == 1 else self.acc[now - 2]
            total = before[self.at[axis]].astype(F32)
            for d in range(1, self.sizes[axis]):
                total = total + self.got[now - 1][d - 1].astype(F32)
            held = self.acc[now - 1]
            held[...] = total.astype(BF16)
        self.done += 1
        if now < stages:
            axis = self.order[now]
            for d in range(1, self.sizes[axis]):
                other = lax.rem(self.at[axis] + d, self.sizes[axis])
                self.copy(held.at[other], self.got[now].at[d - 1], self.device(axis, other))
            return
        mine = self.group(self.rep)
        self.fin[mine] = held[...]
        for other in self.lacking():
            self.copy(held, self.fin.at[mine], (self.patch, other))

    def group(self, rep):
        return rep if "wide" in self.order and "side" in self.order else 0

    def lacking(self):
        return [lax.rem(self.rep + d, self.reps) for d in range(1, self.reps)]

    def finish(self):
        self.arrive()
        for c in self.sent:
            c.wait_send()


class Small(Stream):
    def step(self):
        if self.done < len(self.order):
            return super().step()
        self.arrive()
        axis = self.order[-1]
        total = self.acc[-2][self.at[axis]].astype(F32)
        for d in range(1, self.sizes[axis]):
            total = total + self.got[-1][d - 1].astype(F32)
        self.acc[-1][...] = total.astype(BF16)
        self.fin[self.rep] = self.acc[-1][...]
        for other in self.lacking():
            self.copy(self.acc[-1], self.fin.at[self.rep], (self.patch, other))
        self.done += 1


ORDERS = (
    ("side", "low", "wide", "high"),
    ("side", "wide", "low", "high"),
    ("low", "high"),
    ("side", "low", "wide", "high"),
    ("side", "wide", "low", "high"),
)


def stream_scratch(rows, width, order, sizes):
    lead = tuple(sizes[a] for a in order)
    scratch = [pltpu.VMEM(lead + (rows, width), BF16)]
    slots = sizes["side"] * sizes["wide"] - 1
    for i, axis in enumerate(order):
        scratch.append(pltpu.VMEM((max(sizes[axis] - 1, 1),) + lead[i + 1 :] + (rows, width), BF16))
        slots += sizes[axis] - 1
    for i in range(len(order)):
        scratch.append(pltpu.VMEM(lead[i + 1 :] + (rows, width), BF16))
    scratch.append(pltpu.VMEM((sizes["side"] * sizes["wide"], rows, width), BF16))
    return scratch + [pltpu.SemaphoreType.DMA((slots,)), pltpu.SemaphoreType.DMA((slots,))]


def put(stream, row, value, low=0, rows=None):
    sizes, order = stream.sizes, stream.order
    patches = sizes["low"] * sizes["high"]
    block = value.shape[0] // patches
    rows = block - low if rows is None else rows
    pieces = stream.reps if "side" in order else 1
    width = value.shape[1] // pieces
    for p in range(patches):
        for r in range(pieces):
            at = {"side": r % 2, "wide": r // 2, "low": p % 2, "high": p // 2}
            stream.own[tuple(at[a] for a in order) + (slice(row, row + rows), slice(None))] = value[
                p * block + low : p * block + low + rows, r * width : (r + 1) * width
            ].astype(BF16)


def take(stream, row, rows, out, at, scale):
    if "side" not in stream.order:
        total = stream.fin[0].astype(F32)
        for r in range(1, stream.reps):
            total = total + stream.fin[r].astype(F32)
        out[...] = total * scale
        return
    width = out.shape[1] // stream.reps
    for r in range(stream.reps):
        out[at : at + rows, r * width : (r + 1) * width] = stream.fin[r, row : row + rows, :].astype(F32) * scale


def kernel(
    dims,
    x, e, tgt, w_ein, w_eout, w_nin, w_nout, w_ro, send_ids, far_ids, es, er, count, land, lat,
    o_node, o_edge, o_ein, o_eout, o_nin, o_nout, o_ro,
    near_out, near_in, far_out, far_in, back_near_out, back_near_in, back_far_out, back_far_in,
    xext, xw, table, sgrad, hid, msg, inv, ezg, epg, agg_grad, total,
    near_send, near_recv, far_send, far_recv, bn_send, bn_recv, bf_send, bf_recv,
    *stream_refs,
):
    patches, reps, slot, far, ext, tile = dims
    nodes, width = x.shape
    edges = e.shape[0]
    near = 6 * slot
    patch, rep = lax.axis_index("patch"), lax.axis_index("rep")
    sizes = {"side": 2, "wide": reps // 2, "low": 2, "high": patches // 2}
    streams, used = [], 0
    for order in ORDERS:
        count_refs = 4 + 2 * len(order)
        kind = Stream if "side" in order else Small
        streams.append(kind(stream_refs[used : used + count_refs], order, sizes, patch, rep))
        used += count_refs
    s_in, s_out, s_ro, s_one, s_two = streams

    barrier = pltpu.get_barrier_semaphore()
    for d in range(1, patches):
        pl.semaphore_signal(barrier, inc=1, device_id=(lax.rem(patch + d, patches), rep), device_id_type=MESH)
    for d in range(1, reps):
        pl.semaphore_signal(barrier, inc=1, device_id=(patch, lax.rem(rep + d, reps)), device_id_type=MESH)

    def listed(ids):
        hit = lax.broadcasted_iota(jnp.int32, (nodes, ids.shape[1]), 0) == ids[...]
        return jnp.where(hit, 1.0, 0.0).astype(BF16)

    own_near, own_far = listed(send_ids), listed(far_ids)
    outgoing, outgoing_far = mm_left(own_near, x[...]), mm_left(own_far, x[...])
    for k in range(6):
        near_out[k] = outgoing[k * slot : (k + 1) * slot].astype(BF16)
    for q in range(patches):
        far_out[q] = outgoing_far[q * far : (q + 1) * far].astype(BF16)
    pl.semaphore_wait(barrier, patches - 1 + reps - 1)

    def remote(src, dst, send, recv, device):
        c = pltpu.make_async_remote_copy(
            src_ref=src, dst_ref=dst, send_sem=send, recv_sem=recv, device_id=device, device_id_type=MESH)
        c.start()
        return c

    halo = []
    for k, o in enumerate(OFFSETS):
        to = lax.rem(patch + (o + patches), patches)
        halo.append(remote(near_out.at[k], near_in.at[k], near_send.at[k], near_recv.at[k], (to, rep)))
    for d in range(1, patches):
        to = lax.rem(patch + d, patches)
        halo.append(remote(far_out.at[to], far_in.at[patch], far_send.at[d - 1], far_recv.at[d - 1], (to, rep)))
    far_in[patch] = far_out[patch]

    w_s, w_r, w_e = (w_ein.at[pl.ds(i * width, width)] for i in range(3))
    xext[0:nodes, :] = x[...]
    xw[0:nodes, :] = mm(x[...], w_s[...]).astype(BF16)
    xw[ext : ext + nodes, :] = mm(x[...], w_r[...]).astype(BF16)

    def tables(t, _):
        at = pl.ds(pl.multiple_of(t * tile, tile), tile)
        hit = lax.broadcasted_iota(jnp.int32, (ext, tile), 0) == es[at][None, :]
        table[0:ext, at] = jnp.where(hit, 1.0, 0.0).astype(BF16)
        alive = lax.broadcasted_iota(jnp.int32, (1, tile), 1) + t * tile < count[0]
        ids = jnp.where(alive, er[at][None, :], -1)
        hit = lax.broadcasted_iota(jnp.int32, (nodes, tile), 0) == ids
        table[ext : ext + nodes, at] = jnp.where(hit, 1.0, 0.0).astype(BF16)
        sgrad[at, :] = mm(e[at, :], w_e[...])
        return 0

    lax.fori_loop(0, edges // tile, tables, 0)

    for c in halo:
        c.wait_recv()
    pieces = [near_in[k] for k in range(6)] + [far_in[q] for q in range(patches)]
    pad = ext - nodes - near - patches * far
    if pad:
        pieces.append(jnp.zeros((pad, width), BF16))
    arrived = jnp.concatenate([v.astype(F32) for v in pieces], axis=0).astype(BF16)
    xext[nodes:ext, :] = arrived
    xw[nodes:ext, :] = mm(arrived, w_s[...]).astype(BF16)

    def edge_forward(t, _):
        at = pl.ds(pl.multiple_of(t * tile, tile), tile)
        pre = sgrad[at, :] + mm_left(table[:, at], xw[...])
        s = logistic(pre)
        hidden = (pre * s).astype(BF16)
        sgrad[at, :] = s * (1.0 + pre * (1.0 - s))
        hid[at, :] = hidden
        z = mm(hidden, w_eout[...])
        centred = z - mean(z)
        inverse = lax.rsqrt(mean(centred * centred) + 1e-05)
        inv[at, :] = inverse
        msg[at, :] = (centred * inverse).astype(BF16)
        return 0

    lax.fori_loop(0, edges // tile, edge_forward, 0)

    variables = tgt.shape[1]
    latitude = -0.5 * jnp.pi + (lat[...].astype(F32) + 0.5) * (jnp.pi / BANDS)
    area = jnp.broadcast_to(jnp.cos(latitude)[None, :], (variables, nodes))
    ocean = lax.broadcasted_iota(jnp.int32, (variables, nodes), 0) < OCEAN
    masked = jnp.broadcast_to((land[...])[None, :], (variables, nodes)) == 1
    loss_weight = jnp.transpose(jnp.where(ocean & masked, 0.0, area))
    aggregate = mm(table[ext : ext + nodes, :], msg[...]).astype(BF16)
    node_pre = mm(x[...], w_nin[0:width, :]) + mm(aggregate, w_nin[width : 2 * width, :])
    s = logistic(node_pre)
    node_hidden = (node_pre * s).astype(BF16)
    node_sgrad = s * (1.0 + node_pre * (1.0 - s))
    z = mm(node_hidden, w_nout[...])
    centred = z - mean(z)
    inverse = lax.rsqrt(mean(centred * centred) + 1e-05)
    normed = centred * inverse
    updated = (x[...].astype(F32) + normed).astype(BF16)
    pred_grad = (loss_weight * (mm(updated, w_ro[...]) - tgt[...].astype(F32))).astype(BF16)
    up_grad = mm_right(pred_grad, w_ro[...])
    z_grad = (inverse * (up_grad - mean(up_grad) - normed * mean(up_grad * normed))).astype(BF16)
    pre_grad = (mm_right(z_grad, w_nout[...]) * node_sgrad).astype(BF16)
    total[...] = up_grad + mm_right(pre_grad, w_nin[0:width, :])
    agg_grad[...] = mm_right(pre_grad, w_nin[width : 2 * width, :]).astype(BF16)
    share = width // patches
    put(s_in, 0, jnp.concatenate([mm_left(x[...], pre_grad), mm_left(aggregate, pre_grad)], axis=0))
    s_in.step()
    put(s_out, 0, mm_left(node_hidden, z_grad))
    s_out.step()
    put(s_ro, 0, mm_left(updated, pred_grad))
    s_ro.step()

    def edge_backward(t, _):
        at = pl.ds(pl.multiple_of(t * tile, tile), tile)
        g = mm_left(table[ext : ext + nodes, at], agg_grad[...])
        y = msg[at, :].astype(F32)
        zg = (inv[at, :] * (g - mean(g) - y * mean(g * y))).astype(BF16)
        ezg[at, :] = zg
        epg[at, :] = (mm_right(zg, w_eout[...]) * sgrad[at, :]).astype(BF16)
        return 0

    steps = edges // tile
    cuts = [0, steps // 5, (2 * steps) // 5, (3 * steps) // 5, steps]
    lax.fori_loop(cuts[0], cuts[1], edge_backward, 0)
    s_in.step()
    s_out.step()
    lax.fori_loop(cuts[1], cuts[3], edge_backward, 0)
    s_out.step()
    s_in.step()
    lax.fori_loop(cuts[3], cuts[4], edge_backward, 0)
    s_ro.step()
    s_out.step()
    s_in.step()

    sums32 = mm(table[0:ext, :], epg[...])
    sums = sums32.astype(BF16)
    for k in range(6):
        back_near_out[k] = sums32[nodes + k * slot : nodes + (k + 1) * slot].astype(BF16)
    for q in range(patches):
        at = nodes + near + q * far
        back_far_out[q] = sums32[at : at + far].astype(BF16)
    back = []
    for k, o in enumerate(OFFSETS):
        to = lax.rem(patch + (patches - o), patches)
        back.append(remote(back_near_out.at[k], back_near_in.at[k], bn_send.at[k], bn_recv.at[k], (to, rep)))
    for d in range(1, patches):
        to = lax.rem(patch + d, patches)
        back.append(remote(back_far_out.at[to], back_far_in.at[patch], bf_send.at[d - 1], bf_recv.at[d - 1], (to, rep)))
    back_far_in[patch] = back_far_out[patch]
    rsums = mm(table[ext : ext + nodes, :], epg[...]).astype(BF16)
    put_in = jnp.concatenate(
        [mm_left(xext[...], sums), mm_left(x[...], rsums), mm_left(e[...], epg[...])], axis=0)
    put(s_two, 0, put_in, share)
    s_two.step()
    put(s_one, 0, put_in, 0, share)
    put(s_one, share, mm_left(hid[...], ezg[...]))
    s_one.step()
    s_two.step()
    s_one.step()
    total[...] += mm_right(rsums, w_r[...])

    def edge_out(t, _):
        at = pl.ds(pl.multiple_of(t * tile, tile), tile)
        o_edge[at, :] = mm_right(epg[at, :], w_e[...]).astype(BF16)
        return 0

    lax.fori_loop(0, steps, edge_out, 0)
    s_ro.step()
    s_in.step()
    s_out.step()
    for c in back:
        c.wait_recv()
    near_back = jnp.concatenate([back_near_in[k] for k in range(6)], axis=0)
    far_back = jnp.concatenate([back_far_in[q].astype(F32) for q in range(patches)], axis=0).astype(BF16)
    owned = mm(own_near, near_back) + mm(own_far, far_back)
    owned = (owned + sums32[0:nodes]).astype(BF16)
    o_node[...] = (total[...] + mm_right(owned, w_s[...])).astype(BF16)

    scale = 1.0 / (nodes * patches * reps)
    for _ in range(3):
        s_two.step()
        s_one.step()
    for c in halo + back:
        c.wait_send()
    s_in.finish()
    s_out.finish()
    s_ro.finish()
    take(s_in, 0, 2 * share, o_nin, 0, scale)
    take(s_out, 0, share, o_nout, 0, scale)
    take(s_ro, 0, share, o_ro, 0, scale)
    s_one.finish()
    take(s_one, 0, share, o_ein, 0, scale)
    take(s_one, share, share, o_eout, 0, scale)
    s_two.finish()
    take(s_two, 0, 2 * share, o_ein, share, scale)


def settle_kernel(n, *refs):
    src, dst, held = refs[:n], refs[n : 2 * n], refs[2 * n : 3 * n]
    sem_in, sem_out = refs[3 * n :]
    into = [pltpu.make_async_copy(src[i], held[i], sem_in.at[i]) for i in range(n)]
    out = [pltpu.make_async_copy(held[i], dst[i], sem_out.at[i]) for i in range(n)]
    for c in into:
        c.start()
    for i in range(n):
        into[i].wait()
        out[i].start()
    for c in out:
        c.wait()


def settle(arrays):
    n = len(arrays)
    hbm = pl.BlockSpec(memory_space=pl.ANY)
    return pl.pallas_call(
        functools.partial(settle_kernel, n),
        out_shape=tuple(jax.ShapeDtypeStruct(a.shape, a.dtype) for a in arrays),
        in_specs=[hbm] * n,
        out_specs=tuple([hbm] * n),
        scratch_shapes=[pltpu.VMEM(a.shape, a.dtype) for a in arrays]
        + [pltpu.SemaphoreType.DMA((n,)), pltpu.SemaphoreType.DMA((n,))],
    )(*arrays)


def call(
    node_latents, edge_latents, targets, edge_weight_in, edge_weight_out, node_weight_in, node_weight_out,
    readout_weight, send_rows, far_rows, edge_sender, edge_receiver, edge_count, land_mask, lat_band,
):
    nodes, width = node_latents.shape[1:]
    edges = edge_latents.shape[1]
    variables = targets.shape[2]
    patches, reps = lax.axis_size("patch"), lax.axis_size("rep")
    slot = send_rows.shape[1] // 6
    far = far_rows.shape[1] // patches
    near = 6 * slot
    remote_rows = near + patches * far
    ext = -(-(nodes + remote_rows) // 16) * 16
    tile = 256 if edges % 256 == 0 else 128
    share = width // patches
    vmem = pl.BlockSpec(memory_space=pltpu.VMEM)
    smem = pl.BlockSpec(memory_space=pltpu.SMEM)
    dma = lambda n: pltpu.SemaphoreType.DMA((n,))
    scratch = [
        pltpu.VMEM((6, slot, width), BF16), pltpu.VMEM((6, slot, width), BF16),
        pltpu.VMEM((patches, far, width), BF16), pltpu.VMEM((patches, far, width), BF16),
        pltpu.VMEM((6, slot, width), BF16), pltpu.VMEM((6, slot, width), BF16),
        pltpu.VMEM((patches, far, width), BF16), pltpu.VMEM((patches, far, width), BF16),
        pltpu.VMEM((ext, width), BF16),
        pltpu.VMEM((ext + nodes, width), BF16),
        pltpu.VMEM((ext + nodes, edges), BF16),
        pltpu.VMEM((edges, width), F32),
        pltpu.VMEM((edges, width), BF16),
        pltpu.VMEM((edges, width), BF16),
        pltpu.VMEM((edges, 1), F32),
        pltpu.VMEM((edges, width), BF16),
        pltpu.VMEM((edges, width), BF16),
        pltpu.VMEM((nodes, width), BF16),
        pltpu.VMEM((nodes, width), F32),
        dma(6), dma(6), dma(patches - 1), dma(patches - 1),
        dma(6), dma(6), dma(patches - 1), dma(patches - 1),
    ]
    sizes = {"side": 2, "wide": reps // 2, "low": 2, "high": patches // 2}
    for order, count in zip(ORDERS, (2 * share, share, share, 2 * share, 2 * share)):
        scratch += stream_scratch(count, width // reps if "side" in order else variables, order, sizes)
    shape = jax.ShapeDtypeStruct
    outs = pl.pallas_call(
        functools.partial(kernel, (patches, reps, slot, far, ext, tile)),
        out_shape=(
            shape((nodes, width), BF16), shape((edges, width), BF16),
            shape((3 * share, width), F32), shape((share, width), F32),
            shape((2 * share, width), F32), shape((share, width), F32), shape((share, variables), F32),
        ),
        in_specs=[vmem] * 12 + [smem] + [vmem] * 2,
        out_specs=tuple([vmem] * 7),
        scratch_shapes=scratch,
        compiler_params=pltpu.CompilerParams(
            collective_id=0, has_side_effects=True, vmem_limit_bytes=62 * 1024 * 1024),
    )(
        node_latents[0], edge_latents[0], targets[0], edge_weight_in, edge_weight_out, node_weight_in,
        node_weight_out, readout_weight, send_rows, far_rows, edge_sender, edge_receiver, edge_count,
        land_mask, lat_band,
    )
    outs = settle(outs)
    return (outs[0][None], outs[1][None]) + tuple(outs[2:])


def solution(mesh):
    rows = P("rep", "patch", None)
    in_specs = (rows,) * 3 + (P(),) * 5 + (P("patch", None),) * 2 + (P("patch"),) * 5
    out_specs = (rows,) * 2 + (P("patch", None),) * 5
    return jax.shard_map(call, mesh=mesh, in_specs=in_specs, out_specs=out_specs, check_vma=False)
```

```python
import functools

import jax
import jax.numpy as jnp
from jax import lax
from jax.experimental import pallas as pl
from jax.experimental.pallas import tpu as pltpu
from jax.sharding import PartitionSpec as P

OCEAN = 32
BANDS = 721
OFFSETS = (1, -1, 2, -2, 3, -3)
MESH = pl.DeviceIdType.MESH
F32 = jnp.float32
BF16 = jnp.bfloat16


def mm(left, right):
    return jnp.dot(left, right, preferred_element_type=F32)


def mm_left(left, right):
    return lax.dot_general(left, right, (((0,), (0,)), ((), ())), preferred_element_type=F32)


def mm_right(left, right):
    return lax.dot_general(left, right, (((1,), (1,)), ((), ())), preferred_element_type=F32)


def logistic(values):
    return 1.0 / (1.0 + jnp.exp(-values))


def mean(values):
    return jnp.mean(values, axis=-1, keepdims=True)


class Stream:
    def __init__(self, refs, order, sizes, patch, rep):
        self.order = order
        n = len(order)
        self.own, self.got, self.acc, self.fin = refs[0], refs[1 : 1 + n], refs[1 + n : 1 + 2 * n], refs[1 + 2 * n]
        self.send, self.recv = refs[2 + 2 * n :]
        self.sizes = sizes
        self.patch, self.rep = patch, rep
        self.at = {"side": lax.rem(rep, 2), "wide": lax.div(rep, 2), "low": lax.rem(patch, 2), "high": lax.div(patch, 2)}
        self.reps = sizes["side"] * sizes["wide"]
        self.sent, self.wait, self.slot, self.done = [], [], 0, 0

    def device(self, axis, index):
        at = dict(self.at)
        at[axis] = index
        return (2 * at["high"] + at["low"], 2 * at["wide"] + at["side"])

    def copy(self, src, dst, device):
        c = pltpu.make_async_remote_copy(
            src_ref=src, dst_ref=dst, send_sem=self.send.at[self.slot], recv_sem=self.recv.at[self.slot],
            device_id=device, device_id_type=MESH)
        c.start()
        self.slot += 1
        self.sent.append(c)
        self.wait.append(c)

    def arrive(self):
        for c in self.wait:
            c.wait_recv()
        self.wait = []

    def step(self):
        now, stages = self.done, len(self.order)
        held = self.own
        if now:
            self.arrive()
            axis = self.order[now - 1]
            before = self.own if now == 1 else self.acc[now - 2]
            total = before[self.at[axis]].astype(F32)
            for d in range(1, self.sizes[axis]):
                total = total + self.got[now - 1][d - 1].astype(F32)
            held = self.acc[now - 1]
            held[...] = total.astype(BF16)
        self.done += 1
        if now < stages:
            axis = self.order[now]
            for d in range(1, self.sizes[axis]):
                other = lax.rem(self.at[axis] + d, self.sizes[axis])
                self.copy(held.at[other], self.got[now].at[d - 1], self.device(axis, other))
            return
        mine = self.group(self.rep)
        self.fin[mine] = held[...]
        for other in self.lacking():
            self.copy(held, self.fin.at[mine], (self.patch, other))

    def group(self, rep):
        return rep if "wide" in self.order and "side" in self.order else 0

    def lacking(self):
        return [lax.rem(self.rep + d, self.reps) for d in range(1, self.reps)]

    def finish(self):
        self.arrive()
        for c in self.sent:
            c.wait_send()


class Small(Stream):
    def step(self):
        if self.done < len(self.order):
            return super().step()
        self.arrive()
        axis = self.order[-1]
        total = self.acc[-2][self.at[axis]].astype(F32)
        for d in range(1, self.sizes[axis]):
            total = total + self.got[-1][d - 1].astype(F32)
        self.acc[-1][...] = total.astype(BF16)
        self.fin[self.rep] = self.acc[-1][...]
        for other in self.lacking():
            self.copy(self.acc[-1], self.fin.at[self.rep], (self.patch, other))
        self.done += 1


ORDERS = (
    ("side", "low", "wide", "high"),
    ("side", "wide", "low", "high"),
    ("low", "high"),
    ("side", "low", "wide", "high"),
    ("side", "wide", "low", "high"),
)


def stream_scratch(rows, width, order, sizes):
    lead = tuple(sizes[a] for a in order)
    scratch = [pltpu.VMEM(lead + (rows, width), BF16)]
    slots = sizes["side"] * sizes["wide"] - 1
    for i, axis in enumerate(order):
        scratch.append(pltpu.VMEM((max(sizes[axis] - 1, 1),) + lead[i + 1 :] + (rows, width), BF16))
        slots += sizes[axis] - 1
    for i in range(len(order)):
        scratch.append(pltpu.VMEM(lead[i + 1 :] + (rows, width), BF16))
    scratch.append(pltpu.VMEM((sizes["side"] * sizes["wide"], rows, width), BF16))
    return scratch + [pltpu.SemaphoreType.DMA((slots,)), pltpu.SemaphoreType.DMA((slots,))]


def put(stream, row, value, low=0, rows=None):
    sizes, order = stream.sizes, stream.order
    patches = sizes["low"] * sizes["high"]
    block = value.shape[0] // patches
    rows = block - low if rows is None else rows
    pieces = stream.reps if "side" in order else 1
    width = value.shape[1] // pieces
    for p in range(patches):
        for r in range(pieces):
            at = {"side": r % 2, "wide": r // 2, "low": p % 2, "high": p // 2}
            stream.own[tuple(at[a] for a in order) + (slice(row, row + rows), slice(None))] = value[
                p * block + low : p * block + low + rows, r * width : (r + 1) * width
            ].astype(BF16)


def take(stream, row, rows, out, at, scale):
    if "side" not in stream.order:
        total = stream.fin[0].astype(F32)
        for r in range(1, stream.reps):
            total = total + stream.fin[r].astype(F32)
        out[...] = total * scale
        return
    width = out.shape[1] // stream.reps
    for r in range(stream.reps):
        out[at : at + rows, r * width : (r + 1) * width] = stream.fin[r, row : row + rows, :].astype(F32) * scale


def kernel(
    dims,
    x, e, tgt, w_ein, w_eout, w_nin, w_nout, w_ro, send_ids, far_ids, es, er, count, land, lat,
    o_node, o_edge, o_ein, o_eout, o_nin, o_nout, o_ro,
    near_out, near_in, far_out, far_in, back_near_out, back_near_in, back_far_out, back_far_in,
    xext, xw, table, sgrad, hid, msg, inv, ezg, epg, agg_grad, total,
    near_send, near_recv, far_send, far_recv, bn_send, bn_recv, bf_send, bf_recv,
    *stream_refs,
):
    patches, reps, slot, far, ext, tile = dims
    nodes, width = x.shape
    edges = e.shape[0]
    near = 6 * slot
    patch, rep = lax.axis_index("patch"), lax.axis_index("rep")
    sizes = {"side": 2, "wide": reps // 2, "low": 2, "high": patches // 2}
    streams, used = [], 0
    for order in ORDERS:
        count_refs = 4 + 2 * len(order)
        kind = Stream if "side" in order else Small
        streams.append(kind(stream_refs[used : used + count_refs], order, sizes, patch, rep))
        used += count_refs
    s_in, s_out, s_ro, s_one, s_two = streams

    barrier = pltpu.get_barrier_semaphore()
    for d in range(1, patches):
        pl.semaphore_signal(barrier, inc=1, device_id=(lax.rem(patch + d, patches), rep), device_id_type=MESH)
    for d in range(1, reps):
        pl.semaphore_signal(barrier, inc=1, device_id=(patch, lax.rem(rep + d, reps)), device_id_type=MESH)

    def listed(ids):
        hit = lax.broadcasted_iota(jnp.int32, (nodes, ids.shape[1]), 0) == ids[...]
        return jnp.where(hit, 1.0, 0.0).astype(BF16)

    own_near, own_far = listed(send_ids), listed(far_ids)
    outgoing, outgoing_far = mm_left(own_near, x[...]), mm_left(own_far, x[...])
    for k in range(6):
        near_out[k] = outgoing[k * slot : (k + 1) * slot].astype(BF16)
    for q in range(patches):
        far_out[q] = outgoing_far[q * far : (q + 1) * far].astype(BF16)
    pl.semaphore_wait(barrier, patches - 1 + reps - 1)

    def remote(src, dst, send, recv, device):
        c = pltpu.make_async_remote_copy(
            src_ref=src, dst_ref=dst, send_sem=send, recv_sem=recv, device_id=device, device_id_type=MESH)
        c.start()
        return c

    halo = []
    for k, o in enumerate(OFFSETS):
        to = lax.rem(patch + (o + patches), patches)
        halo.append(remote(near_out.at[k], near_in.at[k], near_send.at[k], near_recv.at[k], (to, rep)))
    for d in range(1, patches):
        to = lax.rem(patch + d, patches)
        halo.append(remote(far_out.at[to], far_in.at[patch], far_send.at[d - 1], far_recv.at[d - 1], (to, rep)))
    far_in[patch] = far_out[patch]

    w_s, w_r, w_e = (w_ein.at[pl.ds(i * width, width)] for i in range(3))
    xext[0:nodes, :] = x[...]
    xw[0:nodes, :] = mm(x[...], w_s[...]).astype(BF16)
    xw[ext : ext + nodes, :] = mm(x[...], w_r[...]).astype(BF16)

    def tables(t, _):
        at = pl.ds(pl.multiple_of(t * tile, tile), tile)
        hit = lax.broadcasted_iota(jnp.int32, (ext, tile), 0) == es[at][None, :]
        table[0:ext, at] = jnp.where(hit, 1.0, 0.0).astype(BF16)
        alive = lax.broadcasted_iota(jnp.int32, (1, tile), 1) + t * tile < count[0]
        ids = jnp.where(alive, er[at][None, :], -1)
        hit = lax.broadcasted_iota(jnp.int32, (nodes, tile), 0) == ids
        table[ext : ext + nodes, at] = jnp.where(hit, 1.0, 0.0).astype(BF16)
        sgrad[at, :] = mm(e[at, :], w_e[...])
        return 0

    lax.fori_loop(0, edges // tile, tables, 0)

    for c in halo:
        c.wait_recv()
    pieces = [near_in[k] for k in range(6)] + [far_in[q] for q in range(patches)]
    pad = ext - nodes - near - patches * far
    if pad:
        pieces.append(jnp.zeros((pad, width), BF16))
    arrived = jnp.concatenate([v.astype(F32) for v in pieces], axis=0).astype(BF16)
    xext[nodes:ext, :] = arrived
    xw[nodes:ext, :] = mm(arrived, w_s[...]).astype(BF16)

    def edge_forward(t, _):
        at = pl.ds(pl.multiple_of(t * tile, tile), tile)
        pre = sgrad[at, :] + mm_left(table[:, at], xw[...])
        s = logistic(pre)
        hidden = (pre * s).astype(BF16)
        sgrad[at, :] = s * (1.0 + pre * (1.0 - s))
        hid[at, :] = hidden
        z = mm(hidden, w_eout[...])
        centred = z - mean(z)
        inverse = lax.rsqrt(mean(centred * centred) + 1e-05)
        inv[at, :] = inverse
        msg[at, :] = (centred * inverse).astype(BF16)
        return 0

    lax.fori_loop(0, edges // tile, edge_forward, 0)

    variables = tgt.shape[1]
    latitude = -0.5 * jnp.pi + (lat[...].astype(F32) + 0.5) * (jnp.pi / BANDS)
    area = jnp.broadcast_to(jnp.cos(latitude)[None, :], (variables, nodes))
    ocean = lax.broadcasted_iota(jnp.int32, (variables, nodes), 0) < OCEAN
    masked = jnp.broadcast_to((land[...])[None, :], (variables, nodes)) == 1
    loss_weight = jnp.transpose(jnp.where(ocean & masked, 0.0, area))
    aggregate = mm(table[ext : ext + nodes, :], msg[...]).astype(BF16)
    node_pre = mm(x[...], w_nin[0:width, :]) + mm(aggregate, w_nin[width : 2 * width, :])
    s = logistic(node_pre)
    node_hidden = (node_pre * s).astype(BF16)
    node_sgrad = s * (1.0 + node_pre * (1.0 - s))
    z = mm(node_hidden, w_nout[...])
    centred = z - mean(z)
    inverse = lax.rsqrt(mean(centred * centred) + 1e-05)
    normed = centred * inverse
    updated = (x[...].astype(F32) + normed).astype(BF16)
    pred_grad = (loss_weight * (mm(updated, w_ro[...]) - tgt[...].astype(F32))).astype(BF16)
    up_grad = mm_right(pred_grad, w_ro[...])
    z_grad = (inverse * (up_grad - mean(up_grad) - normed * mean(up_grad * normed))).astype(BF16)
    pre_grad = (mm_right(z_grad, w_nout[...]) * node_sgrad).astype(BF16)
    total[...] = up_grad + mm_right(pre_grad, w_nin[0:width, :])
    agg_grad[...] = mm_right(pre_grad, w_nin[width : 2 * width, :]).astype(BF16)
    share = width // patches
    put(s_in, 0, jnp.concatenate([mm_left(x[...], pre_grad), mm_left(aggregate, pre_grad)], axis=0))
    s_in.step()
    put(s_out, 0, mm_left(node_hidden, z_grad))
    s_out.step()
    put(s_ro, 0, mm_left(updated, pred_grad))
    s_ro.step()

    def edge_backward(t, _):
        at = pl.ds(pl.multiple_of(t * tile, tile), tile)
        g = mm_left(table[ext : ext + nodes, at], agg_grad[...])
        y = msg[at, :].astype(F32)
        zg = (inv[at, :] * (g - mean(g) - y * mean(g * y))).astype(BF16)
        ezg[at, :] = zg
        epg[at, :] = (mm_right(zg, w_eout[...]) * sgrad[at, :]).astype(BF16)
        return 0

    steps = edges // tile
    cuts = [0, steps // 5, (2 * steps) // 5, (3 * steps) // 5, steps]
    lax.fori_loop(cuts[0], cuts[1], edge_backward, 0)
    s_in.step()
    s_out.step()
    lax.fori_loop(cuts[1], cuts[4], edge_backward, 0)
    s_out.step()
    s_in.step()
    s_ro.step()

    sums32 = mm(table[0:ext, :], epg[...])
    sums = sums32.astype(BF16)
    for k in range(6):
        back_near_out[k] = sums32[nodes + k * slot : nodes + (k + 1) * slot].astype(BF16)
    for q in range(patches):
        at = nodes + near + q * far
        back_far_out[q] = sums32[at : at + far].astype(BF16)
    back = []
    for k, o in enumerate(OFFSETS):
        to = lax.rem(patch + (patches - o), patches)
        back.append(remote(back_near_out.at[k], back_near_in.at[k], bn_send.at[k], bn_recv.at[k], (to, rep)))
    for d in range(1, patches):
        to = lax.rem(patch + d, patches)
        back.append(remote(back_far_out.at[to], back_far_in.at[patch], bf_send.at[d - 1], bf_recv.at[d - 1], (to, rep)))
    back_far_in[patch] = back_far_out[patch]
    rsums = mm(table[ext : ext + nodes, :], epg[...]).astype(BF16)
    put_in = jnp.concatenate(
        [mm_left(xext[...], sums), mm_left(x[...], rsums), mm_left(e[...], epg[...])], axis=0)
    put(s_two, 0, put_in, share)
    s_two.step()
    put(s_one, 0, put_in, 0, share)
    put(s_one, share, mm_left(hid[...], ezg[...]))
    s_one.step()
    s_two.step()
    s_one.step()
    s_out.step()
    s_in.step()
    total[...] += mm_right(rsums, w_r[...])

    def edge_out(t, _):
        at = pl.ds(pl.multiple_of(t * tile, tile), tile)
        o_edge[at, :] = mm_right(epg[at, :], w_e[...]).astype(BF16)
        return 0

    lax.fori_loop(0, steps, edge_out, 0)
    s_ro.step()
    s_in.step()
    s_out.step()
    for c in back:
        c.wait_recv()
    near_back = jnp.concatenate([back_near_in[k] for k in range(6)], axis=0)
    far_back = jnp.concatenate([back_far_in[q].astype(F32) for q in range(patches)], axis=0).astype(BF16)
    owned = mm(own_near, near_back) + mm(own_far, far_back)
    owned = (owned + sums32[0:nodes]).astype(BF16)
    o_node[...] = (total[...] + mm_right(owned, w_s[...])).astype(BF16)

    scale = 1.0 / (nodes * patches * reps)
    for _ in range(3):
        s_two.step()
        s_one.step()
    for c in halo + back:
        c.wait_send()
    s_in.finish()
    s_out.finish()
    s_ro.finish()
    take(s_in, 0, 2 * share, o_nin, 0, scale)
    take(s_out, 0, share, o_nout, 0, scale)
    take(s_ro, 0, share, o_ro, 0, scale)
    s_one.finish()
    take(s_one, 0, share, o_ein, 0, scale)
    take(s_one, share, share, o_eout, 0, scale)
    s_two.finish()
    take(s_two, 0, 2 * share, o_ein, share, scale)


def settle_kernel(n, *refs):
    src, dst, held = refs[:n], refs[n : 2 * n], refs[2 * n : 3 * n]
    sem_in, sem_out = refs[3 * n :]
    into = [pltpu.make_async_copy(src[i], held[i], sem_in.at[i]) for i in range(n)]
    out = [pltpu.make_async_copy(held[i], dst[i], sem_out.at[i]) for i in range(n)]
    for c in into:
        c.start()
    for i in range(n):
        into[i].wait()
        out[i].start()
    for c in out:
        c.wait()


def settle(arrays):
    n = len(arrays)
    hbm = pl.BlockSpec(memory_space=pl.ANY)
    return pl.pallas_call(
        functools.partial(settle_kernel, n),
        out_shape=tuple(jax.ShapeDtypeStruct(a.shape, a.dtype) for a in arrays),
        in_specs=[hbm] * n,
        out_specs=tuple([hbm] * n),
        scratch_shapes=[pltpu.VMEM(a.shape, a.dtype) for a in arrays]
        + [pltpu.SemaphoreType.DMA((n,)), pltpu.SemaphoreType.DMA((n,))],
    )(*arrays)


def call(
    node_latents, edge_latents, targets, edge_weight_in, edge_weight_out, node_weight_in, node_weight_out,
    readout_weight, send_rows, far_rows, edge_sender, edge_receiver, edge_count, land_mask, lat_band,
):
    nodes, width = node_latents.shape[1:]
    edges = edge_latents.shape[1]
    variables = targets.shape[2]
    patches, reps = lax.axis_size("patch"), lax.axis_size("rep")
    slot = send_rows.shape[1] // 6
    far = far_rows.shape[1] // patches
    near = 6 * slot
    remote_rows = near + patches * far
    ext = -(-(nodes + remote_rows) // 16) * 16
    tile = 256 if edges % 256 == 0 else 128
    share = width // patches
    vmem = pl.BlockSpec(memory_space=pltpu.VMEM)
    smem = pl.BlockSpec(memory_space=pltpu.SMEM)
    dma = lambda n: pltpu.SemaphoreType.DMA((n,))
    scratch = [
        pltpu.VMEM((6, slot, width), BF16), pltpu.VMEM((6, slot, width), BF16),
        pltpu.VMEM((patches, far, width), BF16), pltpu.VMEM((patches, far, width), BF16),
        pltpu.VMEM((6, slot, width), BF16), pltpu.VMEM((6, slot, width), BF16),
        pltpu.VMEM((patches, far, width), BF16), pltpu.VMEM((patches, far, width), BF16),
        pltpu.VMEM((ext, width), BF16),
        pltpu.VMEM((ext + nodes, width), BF16),
        pltpu.VMEM((ext + nodes, edges), BF16),
        pltpu.VMEM((edges, width), F32),
        pltpu.VMEM((edges, width), BF16),
        pltpu.VMEM((edges, width), BF16),
        pltpu.VMEM((edges, 1), F32),
        pltpu.VMEM((edges, width), BF16),
        pltpu.VMEM((edges, width), BF16),
        pltpu.VMEM((nodes, width), BF16),
        pltpu.VMEM((nodes, width), F32),
        dma(6), dma(6), dma(patches - 1), dma(patches - 1),
        dma(6), dma(6), dma(patches - 1), dma(patches - 1),
    ]
    sizes = {"side": 2, "wide": reps // 2, "low": 2, "high": patches // 2}
    for order, count in zip(ORDERS, (2 * share, share, share, 2 * share, 2 * share)):
        scratch += stream_scratch(count, width // reps if "side" in order else variables, order, sizes)
    shape = jax.ShapeDtypeStruct
    outs = pl.pallas_call(
        functools.partial(kernel, (patches, reps, slot, far, ext, tile)),
        out_shape=(
            shape((nodes, width), BF16), shape((edges, width), BF16),
            shape((3 * share, width), F32), shape((share, width), F32),
            shape((2 * share, width), F32), shape((share, width), F32), shape((share, variables), F32),
        ),
        in_specs=[vmem] * 12 + [smem] + [vmem] * 2,
        out_specs=tuple([vmem] * 7),
        scratch_shapes=scratch,
        compiler_params=pltpu.CompilerParams(
            collective_id=0, has_side_effects=True, vmem_limit_bytes=62 * 1024 * 1024),
    )(
        node_latents[0], edge_latents[0], targets[0], edge_weight_in, edge_weight_out, node_weight_in,
        node_weight_out, readout_weight, send_rows, far_rows, edge_sender, edge_receiver, edge_count,
        land_mask, lat_band,
    )
    outs = settle(outs)
    return (outs[0][None], outs[1][None]) + tuple(outs[2:])


def solution(mesh):
    rows = P("rep", "patch", None)
    in_specs = (rows,) * 3 + (P(),) * 5 + (P("patch", None),) * 2 + (P("patch"),) * 5
    out_specs = (rows,) * 2 + (P("patch", None),) * 5
    return jax.shard_map(call, mesh=mesh, in_specs=in_specs, out_specs=out_specs, check_vma=False)
```
